32 devices in a mesh: pix: 32 (over z, y, x, core).
Axes of the slice: x: 2, y: 2, z: 4, core: 2. Of those that a mesh axis runs over, the one named last changes fastest.
Arguments:
- green: float32 [2048, 6144], P('pix'), may hold values from -200 to 200, as said below
- sketch: float32 [6144, 128], P('pix'), may hold values from -0.078125 to 0.078125
Outputs:
- basis: float32 [2048, 128], P('pix')
- projection: float32 [6144, 128], P('pix')
- spectrum_gram: float32 [128, 128], replicated
The draws below stay inside these ranges and needn't reach their ends.
Inputs may be any that keep to these rules, and one draw needn't show every extreme that they name: `green`: finite real entries; each patch's column has its own scale.
All inputs are finite; a program needn't handle non-finite values.
Results may differ from the reference program's by a relative error of at most 0.000086.
Values sent between devices are 32-bit elements; how exact they have to be, the bound alone decides.
No kernel may reach another device: no remote copies, remote signals or barrier semaphores. Data moves between devices by JAX's collectives and lax.ppermute only.
A program may use at most 64 MiB of HBM per device.

```python
import jax
import jax.numpy as jnp
from jax import lax

PATCHES = 6144
RANK = 128
PIXELS = 2048


def draw_green(key, part):
    key_cols = jax.random.fold_in(key, 11)
    key_vals = jax.random.fold_in(key, 12)
    col_scale = jnp.exp(jax.random.uniform(key_cols, (1, PATCHES), jnp.float32, jnp.log(0.3), jnp.log(3.0)))
    values = jnp.clip(jax.random.normal(key_vals, (PIXELS, PATCHES), jnp.float32), -6.0, 6.0)
    return values * col_scale


def block_scale(stream_key, shape, pieces, least, largest):
    factor_of, own = 1.0, jax.random.fold_in(stream_key, 6)
    for dim, shards_of in pieces:
        steps = jnp.exp(jax.random.uniform(jax.random.fold_in(own, dim), (shards_of,), jnp.float32, least / len(pieces), largest / len(pieces)))
        factor_of = factor_of * jnp.repeat(steps, shape[dim] // shards_of).reshape([-1 if axis == dim else 1 for axis in range(len(shape))])
    return factor_of


def noise(stream_key, shape, spread, limit, shards=(), kind=jnp.bfloat16):
    values = spread * jax.random.normal(stream_key, shape, jnp.float32)
    if shards:
        values = values * block_scale(stream_key, shape, shards, -0.22, 0.18)
    return jnp.clip(values, -limit, limit).astype(kind)


def setup_inputs(seed: int = 0) -> dict:
    arg_keys = jax.random.split(jax.random.key(seed), 3)
    return {
        "green": draw_green(jax.random.fold_in(arg_keys[2], 71), 0),
        "sketch": noise(arg_keys[1], (PATCHES, RANK), PATCHES ** -0.5, 0.078125, ((0, 32),), jnp.float32),
    }


def reference(green, sketch):
    highest = lax.Precision.HIGHEST
    sketched = jnp.dot(green.astype(jnp.float32), sketch.astype(jnp.float32), precision=highest, preferred_element_type=jnp.float32)
    gram = jnp.dot(sketched.T.astype(jnp.float32), sketched.astype(jnp.float32), precision=highest, preferred_element_type=jnp.float32)
    lower = jnp.linalg.cholesky(gram)
    orthonormal = jax.scipy.linalg.solve_triangular(lower, sketched.T, lower=True).T
    basis = jnp.sqrt(jnp.float32(PIXELS)) * orthonormal
    projection = jnp.dot(green.T.astype(jnp.float32), orthonormal.astype(jnp.float32), precision=highest, preferred_element_type=jnp.float32)
    spectrum_gram = jnp.dot(projection.T.astype(jnp.float32), projection.astype(jnp.float32), precision=highest, preferred_element_type=jnp.float32) / jnp.float32(PATCHES)
    return (basis, projection, spectrum_gram)
```

```python
import jax
import jax.numpy as jnp
from jax import lax
from jax.sharding import PartitionSpec as P

HIGHEST = lax.Precision.HIGHEST
HIGH = lax.Precision.HIGH


def dot(a, b, contract, precision=HIGHEST):
    return lax.dot_general(
        a, b, (contract, ((), ())), precision=precision, preferred_element_type=jnp.float32
    )


def strides(n):
    assert n & (n - 1) == 0
    out = []
    s = 1
    while s < n:
        out.append(s)
        s *= 2
    return out


def swap(x, s, n):
    return lax.ppermute(x, "pix", [(i, i ^ s) for i in range(n)])


def gather_rows(x, me, n):
    rows, cols = x.shape
    b = x[None]
    for s in reversed(strides(n)):
        other = swap(b, s, n)
        bit = (me // s) % 2
        low = jnp.where(bit == 0, b, other)
        high = jnp.where(bit == 0, other, b)
        b = jnp.stack([low, high], axis=1).reshape(-1, rows, cols)
    return b.reshape(-1, cols)


def scatter_sum(x, me, n):
    rows, cols = x.shape
    b = x.reshape(n, rows // n, cols)
    for s in strides(n):
        bit = (me // s) % 2
        pairs = b.reshape(-1, 2, rows // n, cols)
        keep = lax.dynamic_index_in_dim(pairs, bit, 1, False)
        send = lax.dynamic_index_in_dim(pairs, 1 - bit, 1, False)
        b = keep + swap(send, s, n)
    return b[0]


def total(x, n):
    for s in strides(n):
        x = x + swap(x, s, n)
    return x


def body(green, sketch):
    n = lax.axis_size("pix")
    me = lax.axis_index("pix")
    total_pixels = green.shape[0] * n
    patches = green.shape[1]
    sketched = dot(green, gather_rows(sketch, me, n), ((1,), (0,)), HIGH)
    gram = total(dot(sketched, sketched, ((0,), (0,))), n)
    raw = scatter_sum(dot(green, sketched, ((0,), (0,)), HIGH), me, n)
    raw_gram = total(dot(raw, raw, ((0,), (0,))), n)
    lower = jnp.linalg.cholesky(gram)
    inverse = jax.scipy.linalg.solve_triangular(
        lower, jnp.eye(lower.shape[0], dtype=jnp.float32), lower=True
    )
    basis = jnp.sqrt(jnp.float32(total_pixels)) * dot(sketched, inverse, ((1,), (1,)))
    projection = dot(raw, inverse, ((1,), (1,)))
    spectrum = dot(dot(inverse, raw_gram, ((1,), (0,))), inverse, ((1,), (1,)))
    return (basis, projection, spectrum / jnp.float32(patches))


def solution(mesh):
    in_specs = (P("pix", None), P("pix", None))
    out_specs = (P("pix", None), P("pix", None), P())
    return jax.shard_map(body, mesh=mesh, in_specs=in_specs, out_specs=out_specs, check_vma=False)
```

```python
import jax
import jax.numpy as jnp
from jax import lax
from jax.sharding import PartitionSpec as P

HIGHEST = lax.Precision.HIGHEST
HIGH = lax.Precision.HIGH


def dot(a, b, contract, precision=HIGHEST):
    return lax.dot_general(
        a, b, (contract, ((), ())), precision=precision, preferred_element_type=jnp.float32
    )


def swap(x, s, n):
    return lax.ppermute(x, "pix", [(i, i ^ s) for i in range(n)])


def body(green, sketch):
    n = lax.axis_size("pix")
    assert n & (n - 1) == 0 and n >= 8
    me = lax.axis_index("pix")
    pixels, patches = green.shape
    rows, rank = sketch.shape
    top = n // 2
    middle = [1 << k for k in range(1, n.bit_length() - 2)]
    core = me % 2
    high = me // top
    own_half = core == high
    crossing = [(i, i ^ top ^ 1) for i in range(n) if i % 2 != i // top]

    def bit(s):
        return (me // s) % 2

    def cross(x):
        return lax.ppermute(x, "pix", crossing)

    def gather(b, order):
        done = []
        for s in order:
            other = swap(b, s, n)
            axis = sum(d > s for d in done)
            b = jnp.stack(
                [jnp.where(bit(s) == 0, b, other), jnp.where(bit(s) == 0, other, b)], axis=axis
            )
            done.append(s)
        return b

    def scatter(b, order):
        left = sorted(order, reverse=True)
        for s in order:
            axis = left.index(s)
            keep = lax.dynamic_index_in_dim(b, bit(s), axis, False)
            send = lax.dynamic_index_in_dim(b, 1 - bit(s), axis, False)
            b = keep + swap(send, s, n)
            left.remove(s)
        return b

    def total(x, order):
        for s in order:
            x = x + swap(x, s, n)
        return x

    tail = middle[2:][::-1]
    order_a = tail + middle[:2][::-1]
    order_b = tail + middle[:2]

    other = swap(sketch, 1, n)
    pair = jnp.stack([jnp.where(core == 0, sketch, other), jnp.where(core == 0, other, sketch)])
    pair = jnp.where(own_half, pair, cross(pair))
    halves = [gather(pair[0], order_a), gather(pair[1], order_b)]
    block = jnp.stack(halves, axis=-3).reshape(patches // 2, rank)

    half = patches // 2
    first, second = green[:, :half], green[:, half:]
    keep = jnp.where(core == 0, first, second)
    took = swap(jnp.where(core == 0, second, first), 1, n)
    both = jnp.concatenate(
        [jnp.where(core == 0, keep, took), jnp.where(core == 0, took, keep)], axis=0
    )

    part = dot(both, block, ((1,), (0,)), HIGH)
    sketched = part + swap(part, 1, n)
    gram = total(dot(sketched, sketched, ((0,), (0,))), [top] + middle[::-1])

    partial = dot(both, sketched, ((0,), (0,)), HIGH)
    partial = partial.reshape([2] * len(middle) + [2, rows, rank])
    sums = jnp.stack(
        [
            scatter(partial[..., 0, :, :], order_a[::-1]),
            scatter(partial[..., 1, :, :], order_b[::-1]),
        ]
    )
    sums = jnp.where(own_half, sums, cross(sums))
    raw = lax.dynamic_index_in_dim(sums, core, 0, False) + swap(
        lax.dynamic_index_in_dim(sums, 1 - core, 0, False), 1, n
    )
    raw_gram = total(dot(raw, raw, ((0,), (0,))), [1] + middle + [top])

    lower = jnp.linalg.cholesky(gram)
    inverse = jax.scipy.linalg.solve_triangular(lower, jnp.eye(rank, dtype=jnp.float32), lower=True)
    mine = lax.dynamic_slice_in_dim(sketched, core * pixels, pixels, 0)
    basis = jnp.sqrt(jnp.float32(pixels * n)) * dot(mine, inverse, ((1,), (1,)))
    projection = dot(raw, inverse, ((1,), (1,)))
    spectrum = dot(dot(inverse, raw_gram, ((1,), (0,))), inverse, ((1,), (1,)))
    return (basis, projection, spectrum / jnp.float32(patches))


def solution(mesh):
    in_specs = (P("pix", None), P("pix", None))
    out_specs = (P("pix", None), P("pix", None), P())

    return jax.shard_map(body, mesh=mesh, in_specs=in_specs, out_specs=out_specs, check_vma=False)
```

```python
import jax
import jax.numpy as jnp
from jax import lax
from jax.experimental import pallas as pl
from jax.sharding import PartitionSpec as P

HIGHEST = lax.Precision.HIGHEST
HIGH = lax.Precision.HIGH


def dot(a, b, contract, precision=HIGHEST):
    return lax.dot_general(
        a, b, (contract, ((), ())), precision=precision, preferred_element_type=jnp.float32
    )


def swap(x, s, n):
    return lax.ppermute(x, "pix", [(i, i ^ s) for i in range(n)])


def invert_factor_kernel(gram_ref, out_ref):
    rank = gram_ref.shape[0]
    tiles = rank // 8
    rows = lax.broadcasted_iota(jnp.int32, (8, rank), 0)
    lanes = lax.broadcasted_iota(jnp.int32, (8, rank), 1)
    a = [gram_ref[8 * t : 8 * t + 8, :] for t in range(tiles)]
    b = [jnp.where(lanes == rows + 8 * t, 1.0, 0.0).astype(jnp.float32) for t in range(tiles)]

    def spread(x):
        return jnp.broadcast_to(x, (8, rank))

    for t in range(tiles):
        pivots = jnp.ones((8, rank), jnp.float32)
        for r in range(0, 8, 2):
            p = 8 * t + r
            q = p + 1
            app = spread(a[t][r : r + 1, p : p + 1])
            apq = spread(a[t][r : r + 1, q : q + 1])
            aqq = spread(a[t][r + 1 : r + 2, q : q + 1])
            inv_p = 1.0 / app
            step = apq * inv_p
            left = aqq - apq * step
            inv_q = 1.0 / left
            pivots = jnp.where(rows == r, app, jnp.where(rows == r + 1, left, pivots))
            row_p, row_q = spread(a[t][r : r + 1, :]), spread(a[t][r + 1 : r + 2, :])
            row_q = row_q - step * row_p
            low_p, low_q = spread(b[t][r : r + 1, :]), spread(b[t][r + 1 : r + 2, :])
            low_q = low_q - step * low_p
            for u in range(t, tiles):
                col_p, col_q = spread(a[u][:, p : p + 1]), spread(a[u][:, q : q + 1])
                f = col_p * inv_p
                g = (col_q - f * apq) * inv_q
                if u == t:
                    f = jnp.where(rows > r, f, 0.0)
                    g = jnp.where(rows > r + 1, g, 0.0)
                b[u] = b[u] - f * low_p - g * low_q
                if u > t or r < 6:
                    a[u] = a[u] - f * row_p - g * row_q
        out_ref[8 * t : 8 * t + 8, :] = b[t] * lax.rsqrt(pivots)


def invert_factor(gram):
    return pl.pallas_call(
        invert_factor_kernel, out_shape=jax.ShapeDtypeStruct(gram.shape, jnp.float32)
    )(gram)


def body(green, sketch):
    n = lax.axis_size("pix")
    assert n & (n - 1) == 0 and n >= 8
    me = lax.axis_index("pix")
    pixels, patches = green.shape
    rows, rank = sketch.shape
    top = n // 2
    middle = [1 << k for k in range(1, n.bit_length() - 2)]
    core = me % 2
    high = me // top
    own_half = core == high
    crossing = [(i, i ^ top ^ 1) for i in range(n) if i % 2 != i // top]

    def bit(s):
        return (me // s) % 2

    def cross(x):
        return lax.ppermute(x, "pix", crossing)

    def gather(b, order):
        done = []
        for s in order:
            other = swap(b, s, n)
            axis = sum(d > s for d in done)
            b = jnp.stack(
                [jnp.where(bit(s) == 0, b, other), jnp.where(bit(s) == 0, other, b)], axis=axis
            )
            done.append(s)
        return b

    def scatter(b, order):
        left = sorted(order, reverse=True)
        for s in order:
            axis = left.index(s)
            keep = lax.dynamic_index_in_dim(b, bit(s), axis, False)
            send = lax.dynamic_index_in_dim(b, 1 - bit(s), axis, False)
            b = keep + swap(send, s, n)
            left.remove(s)
        return b

    def total(x, order):
        for s in order:
            x = x + swap(x, s, n)
        return x

    tail = middle[2:][::-1]
    order_a = tail + middle[:2][::-1]
    order_b = tail + middle[:2]

    other = swap(sketch, 1, n)
    pair = jnp.stack([jnp.where(core == 0, sketch, other), jnp.where(core == 0, other, sketch)])
    pair = jnp.where(own_half, pair, cross(pair))
    halves = [gather(pair[0], order_a), gather(pair[1], order_b)]
    block = jnp.stack(halves, axis=-3).reshape(patches // 2, rank)

    half = patches // 2
    first, second = green[:, :half], green[:, half:]
    keep = jnp.where(core == 0, first, second)
    took = swap(jnp.where(core == 0, second, first), 1, n)
    both = jnp.concatenate(
        [jnp.where(core == 0, keep, took), jnp.where(core == 0, took, keep)], axis=0
    )

    part = dot(both, block, ((1,), (0,)), HIGH)
    sketched = part + swap(part, 1, n)
    gram = total(dot(sketched, sketched, ((0,), (0,))), [top] + middle[::-1])

    partial = dot(both, sketched, ((0,), (0,)), HIGH)
    partial = partial.reshape([2] * len(middle) + [2, rows, rank])
    sums = jnp.stack(
        [
            scatter(partial[..., 0, :, :], order_a[::-1]),
            scatter(partial[..., 1, :, :], order_b[::-1]),
        ]
    )
    sums = sums + swap(sums, top, n)
    summed = sums.reshape(2 * rows, rank)
    raw_gram = total(dot(summed, summed, ((0,), (0,))), [1] + middle)
    handed = swap(lax.dynamic_index_in_dim(sums, 1 - core, 0, False), 1, n)
    raw = jnp.where(own_half, lax.dynamic_index_in_dim(sums, core, 0, False), handed)

    inverse = invert_factor(gram)
    mine = lax.dynamic_slice_in_dim(sketched, core * pixels, pixels, 0)
    basis = jnp.sqrt(jnp.float32(pixels * n)) * dot(mine, inverse, ((1,), (1,)))
    projection = dot(raw, inverse, ((1,), (1,)))
    spectrum = dot(dot(inverse, raw_gram, ((1,), (0,))), inverse, ((1,), (1,)))
    return (basis, projection, spectrum / jnp.float32(patches))


def solution(mesh):
    in_specs = (P("pix", None), P("pix", None))
    out_specs = (P("pix", None), P("pix", None), P())

    return jax.shard_map(body, mesh=mesh, in_specs=in_specs, out_specs=out_specs, check_vma=False)
```
